32 devices in a mesh: row: 8 (over y, x, core), col: 4 (over z).
Axes of the slice: x: 2, y: 2, z: 4, core: 2. Of those that a mesh axis runs over, the one named last changes fastest.
Arguments:
- species: float32 [4, 64, 32, 256], P(None, None, 'row', 'col'), may hold values from -6 to 6
- symbol_x: float32 [64], replicated, may hold values from 0.3 to 3
- symbol_y: float32 [32], replicated, may hold values from 0.3 to 3
- symbol_z: float32 [256], replicated, may hold values from 0.3 to 3
Outputs:
- coefficients: float32 [4, 64, 32, 256], P(None, 'row', 'col')
The draws below stay inside these ranges and needn't reach their ends.
All inputs are finite; a program needn't handle non-finite values.
Results may differ from the reference program's by a relative error of at most 0.00007.
Values sent between devices are 32-bit elements; how exact they have to be, the bound alone decides.
No kernel may reach another device: no remote copies, remote signals or barrier semaphores. Data moves between devices by JAX's collectives and lax.ppermute only.
A program may use at most 64 MiB of HBM per device.

```python
import jax
import jax.numpy as jnp
from jax import lax

GRID_X = 64
GRID_Y = 32
GRID_Z = 256
FIELDS = 4


def levels(key, extent, split, smallest, largest):
    def one(axis_at, parts):
        draws = jax.random.uniform(jax.random.fold_in(jax.random.fold_in(key, 6), axis_at), (parts,), jnp.float32, smallest / len(split), largest / len(split))
        return jnp.repeat(jnp.exp(draws), extent[axis_at] // parts).reshape((-1,) + (1,) * (len(extent) - axis_at - 1))

    factor_of = one(*split[0])
    for cut in split[1:]:
        factor_of = factor_of * one(*cut)
    return factor_of


def bell_draw(key, shape, width, bound, pieces=(), kind=jnp.bfloat16):
    array = width * jax.random.normal(key, shape, jnp.float32)
    if pieces:
        array = array * levels(key, shape, pieces, -0.22, 0.18)
    return jnp.clip(array, -bound, bound).astype(kind)


def setup_inputs(seed: int = 0) -> dict:
    key_of = jax.random.split(jax.random.key(seed), 5)
    species = bell_draw(key_of[0], (FIELDS, GRID_X, GRID_Y, GRID_Z), 1.0, 6.0, ((2, 8), (3, 4)), jnp.float32)
    symbol_x = jnp.clip(jax.random.uniform(key_of[1], (GRID_X,), jnp.float32, 0.3, 3.0), 0.3, 3.0)
    symbol_y = jnp.clip(jax.random.uniform(key_of[2], (GRID_Y,), jnp.float32, 0.3, 3.0), 0.3, 3.0)
    symbol_z = jnp.clip(jax.random.uniform(key_of[3], (GRID_Z,), jnp.float32, 0.3, 3.0), 0.3, 3.0)
    return dict(species=species, symbol_x=symbol_x, symbol_y=symbol_y, symbol_z=symbol_z)


def transform_table(count):
    rank = jnp.arange(count)
    angle = (jnp.pi / (count + 1)) * (((rank[:, None] + 1) * (rank[None, :] + 1)) % (2 * count + 2)).astype(jnp.float32)
    return jnp.sin(angle) * (2.0 / (count + 1)) ** 0.5


def transform_dim(values, dim):
    moved = jnp.tensordot(values, transform_table(values.shape[dim]), axes=([dim], [0]), precision=lax.Precision.HIGHEST)
    return jnp.moveaxis(moved, -1, dim)


def reference(species, symbol_x, symbol_y, symbol_z):
    coefficients = species
    coefficients = transform_dim(coefficients, 1)
    coefficients = transform_dim(coefficients, 2)
    coefficients = transform_dim(coefficients, 3)
    symbol = symbol_x[:, None, None] + symbol_y[None, :, None] + symbol_z[None, None, :]
    coefficients = coefficients / symbol
    return coefficients
```

```python
import functools

import jax
import jax.numpy as jnp
import numpy as np
from jax import lax
from jax.experimental import pallas as pl
from jax.experimental.pallas import tpu as pltpu
from jax.sharding import PartitionSpec as P


LANES = 128
VMEM = 6 << 20
DIRECT = 16


def sine_table(count):
    rank = np.arange(1, count + 1)
    angle = np.pi / (count + 1) * (np.outer(rank, rank) % (2 * count + 2))
    return (np.sin(angle) * np.sqrt(2.0 / (count + 1))).astype(np.float32)


def two_terms(table):
    high = table.astype(jnp.bfloat16)
    low = (table - high.astype(np.float32)).astype(jnp.bfloat16)
    return high, low


def split(values):
    high = values.astype(jnp.bfloat16)
    low = (values - high.astype(jnp.float32)).astype(jnp.bfloat16)
    return high, low


def dot(left, right):
    return lax.dot_general(
        left, right, (((1,), (0,)), ((), ())), preferred_element_type=jnp.float32
    )


def dot3(left, right):
    return dot(left[0], right[0]) + dot(left[0], right[1]) + dot(left[1], right[0])


def x_kernel(at_ref, a_ref, th_ref, tl_ref, *out_refs):
    me = at_ref[0]
    fields = a_ref.shape[0]
    a = jnp.concatenate([a_ref[f] for f in range(fields)], axis=-1)
    right = split(a)
    count = len(out_refs)
    left = tuple(
        jnp.concatenate([t[me ^ k] for k in range(count)], axis=0) for t in (th_ref, tl_ref)
    )
    out = dot3(left, right)
    share = out.shape[0] // count
    for k, ref in enumerate(out_refs):
        ref[...] = out[k * share : (k + 1) * share]


def y_kernel(at_ref, *refs, rows, cols):
    piece_refs = refs[:rows]
    th_ref, tl_ref = refs[rows : rows + 2]
    out_refs = refs[rows + 2 : rows + 2 + cols]
    ch_ref, cl_ref = refs[rows + 2 + cols :]
    me_r, me_c = at_ref[0], at_ref[1]
    for k, ref in enumerate(piece_refs):
        high, low = split(ref[...])
        ch_ref[me_r ^ k] = high
        cl_ref[me_r ^ k] = low
    width = ch_ref.shape[-1]
    right = tuple(r[...].reshape(-1, width) for r in (ch_ref, cl_ref))
    left = tuple(
        jnp.concatenate([t[me_c ^ k] for k in range(cols)], axis=0) for t in (th_ref, tl_ref)
    )
    out = dot3(left, right)
    share = out.shape[0] // cols
    for k, ref in enumerate(out_refs):
        ref[...] = out[k * share : (k + 1) * share]


def z_kernel(at_ref, sx_ref, sy_ref, *refs, cols, fields):
    piece_refs = refs[:cols]
    sz_ref, th_ref, tl_ref, out_ref = refs[cols:]
    me_r, me_c = at_ref[0], at_ref[1]
    share_x, share_y = out_ref.shape[1], out_ref.shape[2]
    part_z = piece_refs[0].shape[-1] // fields
    pieces = [ref[...] for ref in piece_refs]
    a = jnp.concatenate(
        [
            jnp.concatenate([p[:, f * part_z : (f + 1) * part_z] for p in pieces], axis=-1)
            for f in range(fields)
        ],
        axis=0,
    )
    left = split(a)
    right = tuple(
        jnp.concatenate([t[me_c ^ k] for k in range(cols)], axis=0) for t in (th_ref, tl_ref)
    )
    out = dot3(left, right)
    out = out.reshape(fields, share_x, share_y, out.shape[-1])
    place = lax.broadcasted_iota(jnp.int32, (share_y, 1), 0)
    part_y = jnp.zeros((share_y, 1), jnp.float32)
    for j in range(share_y):
        part_y = jnp.where(place == j, sy_ref[me_c * share_y + j], part_y)
    yz = part_y + sz_ref[...]
    for i in range(share_x):
        inverse = 1.0 / (yz + sx_ref[me_r * share_x + i])
        for f in range(fields):
            out_ref[f, i] = out[f, i] * inverse


def exchange(pieces, axis, count):
    return [pieces[0]] + [
        lax.ppermute(pieces[k], axis, [(i, i ^ k) for i in range(count)])
        for k in range(1, count)
    ]


def fast(species, symbol_x, symbol_y, symbol_z, *, rows, cols):
    fields, all_x, part_y, part_z = species.shape
    all_y, all_z = part_y * rows, part_z * cols
    share_x, share_y = all_x // rows, all_y // cols
    width = fields * part_z
    at = jnp.stack([lax.axis_index("row"), lax.axis_index("col")]).astype(jnp.int32)
    vmem = pl.BlockSpec(memory_space=pltpu.VMEM)
    smem = pl.BlockSpec(memory_space=pltpu.SMEM)

    table_x = np.kron(sine_table(all_x), np.eye(part_y, dtype=np.float32))
    table_x = table_x.reshape(rows, share_x * part_y, all_x * part_y)
    table_y = sine_table(all_y).reshape(cols, share_y, rows, part_y)
    table_y = np.einsum("cjry,ab->cajrby", table_y, np.eye(share_x, dtype=np.float32))
    table_y = table_y.reshape(cols, share_x * share_y, rows * share_x * part_y)
    table_z = sine_table(all_z).reshape(cols, part_z, all_z)

    piece = jax.ShapeDtypeStruct((share_x * part_y, width), jnp.float32)
    pieces = pl.pallas_call(
        x_kernel,
        out_shape=[piece] * rows,
        in_specs=[smem, vmem, vmem, vmem],
        out_specs=[vmem] * rows,
        compiler_params=pltpu.CompilerParams(vmem_limit_bytes=VMEM),
        name="x_modes",
    )(at, species.reshape(fields, all_x * part_y, part_z), *two_terms(table_x))
    pieces = exchange(pieces, "row", rows)

    block = jax.ShapeDtypeStruct((share_x * share_y, width), jnp.float32)
    line = pltpu.VMEM((rows, share_x * part_y, width), jnp.bfloat16)
    blocks = pl.pallas_call(
        functools.partial(y_kernel, rows=rows, cols=cols),
        out_shape=[block] * cols,
        in_specs=[smem] + [vmem] * (rows + 2),
        out_specs=[vmem] * cols,
        scratch_shapes=[line, line],
        compiler_params=pltpu.CompilerParams(vmem_limit_bytes=VMEM),
        name="y_modes",
    )(at, *pieces, *two_terms(table_y))
    blocks = exchange(blocks, "col", cols)

    return pl.pallas_call(
        functools.partial(z_kernel, cols=cols, fields=fields),
        out_shape=jax.ShapeDtypeStruct((fields, share_x, share_y, all_z), jnp.float32),
        in_specs=[smem] * 3 + [vmem] * (cols + 3),
        out_specs=vmem,
        compiler_params=pltpu.CompilerParams(vmem_limit_bytes=VMEM),
        name="z_modes",
    )(at, symbol_x, symbol_y, *blocks, symbol_z[None], *two_terms(table_z))


def plain_transform(values, dim):
    table = jnp.asarray(sine_table(values.shape[dim]))
    moved = jnp.tensordot(values, table, axes=([dim], [0]), precision=lax.Precision.HIGHEST)
    return jnp.moveaxis(moved, -1, dim)


def plain(species, symbol_x, symbol_y, symbol_z):
    values = plain_transform(species, 1)
    values = lax.all_to_all(values, "row", split_axis=1, concat_axis=2, tiled=True)
    values = plain_transform(values, 2)
    values = lax.all_to_all(values, "col", split_axis=2, concat_axis=3, tiled=True)
    values = plain_transform(values, 3)
    share_x, share_y = values.shape[1], values.shape[2]
    part_x = lax.dynamic_slice_in_dim(symbol_x, lax.axis_index("row") * share_x, share_x)
    part_y = lax.dynamic_slice_in_dim(symbol_y, lax.axis_index("col") * share_y, share_y)
    return values / (part_x[:, None, None] + part_y[None, :, None] + symbol_z)


def solution(mesh):
    rows, cols = mesh.shape["row"], mesh.shape["col"]

    def on_device(species, symbol_x, symbol_y, symbol_z):
        direct = all(n <= DIRECT and n & (n - 1) == 0 for n in (rows, cols))
        if direct and species.shape[3] * species.shape[0] % LANES == 0:
            return fast(species, symbol_x, symbol_y, symbol_z, rows=rows, cols=cols)
        return plain(species, symbol_x, symbol_y, symbol_z)

    return jax.shard_map(
        on_device,
        mesh=mesh,
        in_specs=(P(None, None, "row", "col"), P(), P(), P()),
        out_specs=P(None, "row", "col", None),
        check_vma=False,
    )
```

```python
import functools

import jax
import jax.numpy as jnp
import numpy as np
from jax import lax
from jax.experimental import pallas as pl
from jax.experimental.pallas import tpu as pltpu
from jax.sharding import PartitionSpec as P


LANES = 128
VMEM = 6 << 20
DIRECT = 16


def sine_table(count):
    rank = np.arange(1, count + 1)
    angle = np.pi / (count + 1) * (np.outer(rank, rank) % (2 * count + 2))
    return (np.sin(angle) * np.sqrt(2.0 / (count + 1))).astype(np.float32)


def two_terms(table):
    high = table.astype(jnp.bfloat16)
    low = (table - high.astype(np.float32)).astype(jnp.bfloat16)
    return np.stack([high, low])


def split(values):
    high = values.astype(jnp.bfloat16)
    low = (values - high.astype(jnp.float32)).astype(jnp.bfloat16)
    return high, low


def dot(left, right):
    return lax.dot_general(
        left, right, (((1,), (0,)), ((), ())), preferred_element_type=jnp.float32
    )


def dot3(left, right):
    return dot(left[0], right[0]) + dot(left[0], right[1]) + dot(left[1], right[0])


def start_order(count):
    return [0, *range(count - 1, 0, -1)]


def x_kernel(species_ref, table_ref, *refs, order):
    out_refs, (a_ref, t_ref, sems) = refs[: len(order)], refs[len(order) :]
    me = lax.axis_index("row")
    fields = a_ref.shape[0]
    table = pltpu.make_async_copy(table_ref, t_ref, sems.at[fields])
    table.start()
    copies = [
        pltpu.make_async_copy(species_ref.at[f], a_ref.at[f], sems.at[f]) for f in range(fields)
    ]
    for copy in copies:
        copy.start()
    share = t_ref.shape[2]
    part = a_ref.shape[2]
    step = min(fields, max(1, LANES // part))
    table.wait()
    left = tuple(jnp.concatenate([t_ref[i, me ^ k] for k in order], axis=0) for i in range(2))
    for f in range(0, fields, step):
        for copy in copies[f : f + step]:
            copy.wait()
        a = jnp.concatenate([a_ref[g] for g in range(f, f + step)], axis=-1)
        out = dot3(left, split(a))
        for n, ref in enumerate(out_refs):
            ref[:, f * part : (f + step) * part] = out[n * share : (n + 1) * share]


def y_kernel(*refs, row_order, col_order):
    rows, cols = len(row_order), len(col_order)
    piece_refs = refs[:rows]
    t_ref = refs[rows]
    out_refs = refs[rows + 1 : rows + 1 + cols]
    ch_ref, cl_ref = refs[rows + 1 + cols :]
    me_r, me_c = lax.axis_index("row"), lax.axis_index("col")
    for k, ref in zip(row_order, piece_refs):
        high, low = split(ref[...])
        ch_ref[me_r ^ k] = high
        cl_ref[me_r ^ k] = low
    width = ch_ref.shape[-1]
    right = tuple(r[...].reshape(-1, width) for r in (ch_ref, cl_ref))
    left = tuple(jnp.concatenate([t_ref[i, me_c ^ k] for k in col_order], axis=0) for i in range(2))
    out = dot3(left, right)
    share = out.shape[0] // cols
    for n, ref in enumerate(out_refs):
        ref[...] = out[n * share : (n + 1) * share]


def symbol_kernel(sx_ref, sy_ref, sz_ref, out_ref):
    share_x, share_y = out_ref.shape[0], out_ref.shape[1]
    at_x = lax.axis_index("row") * share_x
    at_y = lax.axis_index("col") * share_y
    place = lax.broadcasted_iota(jnp.int32, (share_y, 1), 0)
    part_y = jnp.zeros((share_y, 1), jnp.float32)
    for j in range(share_y):
        part_y = jnp.where(place == j, sy_ref[at_y + j], part_y)
    yz = part_y + sz_ref[...]
    for i in range(share_x):
        out_ref[i] = 1.0 / (yz + sx_ref[at_x + i])


def z_kernel(*refs, order, fields):
    cols = len(order)
    piece_refs = refs[:cols]
    inverse_ref, t_ref, out_ref, o_ref, sems = refs[cols:]
    me = lax.axis_index("col")
    share_x, share_y, all_z = inverse_ref.shape
    part = piece_refs[0].shape[-1] // fields
    right = tuple(jnp.concatenate([t_ref[i, me ^ k] for k in order], axis=0) for i in range(2))
    inverse = inverse_ref[...]
    copies = []
    for f in range(fields):
        a = jnp.concatenate([r[:, f * part : (f + 1) * part] for r in piece_refs], axis=-1)
        out = dot3(split(a), right)
        o_ref[f] = out.reshape(share_x, share_y, all_z) * inverse
        copies.append(pltpu.make_async_copy(o_ref.at[f], out_ref.at[f], sems.at[f]))
        copies[-1].start()
    for copy in copies:
        copy.wait()


def exchange(pieces, axis, order):
    count = len(order)
    return [
        lax.ppermute(piece, axis, [(i, i ^ k) for i in range(count)]) if k else piece
        for k, piece in zip(order, pieces)
    ]


def fast(species, symbol_x, symbol_y, symbol_z, *, rows, cols):
    fields, all_x, part_y, part_z = species.shape
    all_y, all_z = part_y * rows, part_z * cols
    share_x, share_y = all_x // rows, all_y // cols
    width = fields * part_z
    row_order, col_order = start_order(rows), start_order(cols)
    vmem = pl.BlockSpec(memory_space=pltpu.VMEM)
    smem = pl.BlockSpec(memory_space=pltpu.SMEM)
    hbm = pl.BlockSpec(memory_space=pltpu.HBM)
    params = pltpu.CompilerParams(vmem_limit_bytes=VMEM)

    table_x = np.kron(sine_table(all_x), np.eye(part_y, dtype=np.float32))
    table_x = table_x.reshape(rows, share_x * part_y, all_x * part_y)
    table_y = sine_table(all_y).reshape(cols, share_y, rows, part_y)
    table_y = np.einsum("cjry,ab->cajrby", table_y, np.eye(share_x, dtype=np.float32))
    table_y = table_y.reshape(cols, share_x * share_y, rows * share_x * part_y)
    table_z = sine_table(all_z).reshape(cols, part_z, all_z)
    table_x, table_y, table_z = two_terms(table_x), two_terms(table_y), two_terms(table_z)

    piece = jax.ShapeDtypeStruct((share_x * part_y, width), jnp.float32)
    pieces = pl.pallas_call(
        functools.partial(x_kernel, order=row_order),
        out_shape=[piece] * rows,
        in_specs=[hbm, hbm],
        out_specs=[vmem] * rows,
        scratch_shapes=[
            pltpu.VMEM((fields, all_x * part_y, part_z), jnp.float32),
            pltpu.VMEM(table_x.shape, jnp.bfloat16),
            pltpu.SemaphoreType.DMA((fields + 1,)),
        ],
        compiler_params=params,
        name="x_modes",
    )(
        pltpu.with_memory_space_constraint(
            species.reshape(fields, all_x * part_y, part_z), pltpu.HBM
        ),
        pltpu.with_memory_space_constraint(jnp.asarray(table_x), pltpu.HBM),
    )
    pieces = exchange(pieces, "row", row_order)

    block = jax.ShapeDtypeStruct((share_x * share_y, width), jnp.float32)
    line = pltpu.VMEM((rows, share_x * part_y, width), jnp.bfloat16)
    blocks = pl.pallas_call(
        functools.partial(y_kernel, row_order=row_order, col_order=col_order),
        out_shape=[block] * cols,
        in_specs=[vmem] * (rows + 1),
        out_specs=[vmem] * cols,
        scratch_shapes=[line, line],
        compiler_params=params,
        name="y_modes",
    )(*pieces, table_y)
    blocks = exchange(blocks, "col", col_order)

    inverse = pl.pallas_call(
        symbol_kernel,
        out_shape=jax.ShapeDtypeStruct((share_x, share_y, all_z), jnp.float32),
        in_specs=[smem, smem, vmem],
        out_specs=vmem,
        compiler_params=params,
        name="inverse_symbol",
    )(symbol_x, symbol_y, symbol_z[None])
    return pl.pallas_call(
        functools.partial(z_kernel, order=col_order, fields=fields),
        out_shape=jax.ShapeDtypeStruct((fields, share_x, share_y, all_z), jnp.float32),
        in_specs=[vmem] * (cols + 2),
        out_specs=hbm,
        scratch_shapes=[
            pltpu.VMEM((fields, share_x, share_y, all_z), jnp.float32),
            pltpu.SemaphoreType.DMA((fields,)),
        ],
        compiler_params=params,
        name="z_modes",
    )(*blocks, inverse, table_z)


def plain_transform(values, dim):
    table = jnp.asarray(sine_table(values.shape[dim]))
    moved = jnp.tensordot(values, table, axes=([dim], [0]), precision=lax.Precision.HIGHEST)
    return jnp.moveaxis(moved, -1, dim)


def plain(species, symbol_x, symbol_y, symbol_z):
    values = plain_transform(species, 1)
    values = lax.all_to_all(values, "row", split_axis=1, concat_axis=2, tiled=True)
    values = plain_transform(values, 2)
    values = lax.all_to_all(values, "col", split_axis=2, concat_axis=3, tiled=True)
    values = plain_transform(values, 3)
    share_x, share_y = values.shape[1], values.shape[2]
    part_x = lax.dynamic_slice_in_dim(symbol_x, lax.axis_index("row") * share_x, share_x)
    part_y = lax.dynamic_slice_in_dim(symbol_y, lax.axis_index("col") * share_y, share_y)
    return values / (part_x[:, None, None] + part_y[None, :, None] + symbol_z)


def solution(mesh):
    rows, cols = mesh.shape["row"], mesh.shape["col"]

    def on_device(species, symbol_x, symbol_y, symbol_z):
        direct = all(n <= DIRECT and n & (n - 1) == 0 for n in (rows, cols))
        if direct and species.shape[3] * species.shape[0] % LANES == 0:
            return fast(species, symbol_x, symbol_y, symbol_z, rows=rows, cols=cols)
        return plain(species, symbol_x, symbol_y, symbol_z)

    return jax.shard_map(
        on_device,
        mesh=mesh,
        in_specs=(P(None, None, "row", "col"), P(), P(), P()),
        out_specs=P(None, "row", "col", None),
        check_vma=False,
    )
```

```python
import functools

import jax
import jax.numpy as jnp
import numpy as np
from jax import lax
from jax.experimental import pallas as pl
from jax.experimental.pallas import tpu as pltpu
from jax.sharding import PartitionSpec as P


LANES = 128
VMEM = 6 << 20
DIRECT = 16


def sine_table(count):
    rank = np.arange(1, count + 1)
    angle = np.pi / (count + 1) * (np.outer(rank, rank) % (2 * count + 2))
    return (np.sin(angle) * np.sqrt(2.0 / (count + 1))).astype(np.float32)


def two_terms(table):
    high = table.astype(jnp.bfloat16)
    low = (table - high.astype(np.float32)).astype(jnp.bfloat16)
    return np.stack([high, low])


def split(values):
    high = values.astype(jnp.bfloat16)
    low = (values - high.astype(jnp.float32)).astype(jnp.bfloat16)
    return high, low


def dot(left, right):
    return lax.dot_general(
        left, right, (((1,), (0,)), ((), ())), preferred_element_type=jnp.float32
    )


def dot3(left, right):
    return dot(left[0], right[0]) + dot(left[0], right[1]) + dot(left[1], right[0])


def x_kernel(species_ref, table_ref, *refs, order):
    out_refs, (a_ref, t_ref, sems) = refs[: len(order)], refs[len(order) :]
    me = lax.axis_index("row")
    fields = a_ref.shape[0]
    table = pltpu.make_async_copy(table_ref, t_ref, sems.at[fields])
    table.start()
    copies = [
        pltpu.make_async_copy(species_ref.at[f], a_ref.at[f], sems.at[f]) for f in range(fields)
    ]
    for copy in copies:
        copy.start()
    share = t_ref.shape[2]
    table.wait()
    left = tuple(jnp.concatenate([t_ref[i, me ^ k] for k in order], axis=0) for i in range(2))
    for copy in copies:
        copy.wait()
    out = dot3(left, split(jnp.concatenate([a_ref[f] for f in range(fields)], axis=-1)))
    for n, ref in enumerate(out_refs):
        ref[...] = out[n * share : (n + 1) * share]


def y_kernel(*refs, row_order, col_order):
    rows, cols = len(row_order), len(col_order)
    piece_refs = refs[:rows]
    t_ref = refs[rows]
    out_refs = refs[rows + 1 : rows + 1 + cols]
    ch_ref, cl_ref = refs[rows + 1 + cols :]
    me_r, me_c = lax.axis_index("row"), lax.axis_index("col")
    for k, ref in zip(row_order, piece_refs):
        high, low = split(ref[...])
        ch_ref[me_r ^ k] = high
        cl_ref[me_r ^ k] = low
    width = ch_ref.shape[-1]
    right = tuple(r[...].reshape(-1, width) for r in (ch_ref, cl_ref))
    left = tuple(jnp.concatenate([t_ref[i, me_c ^ k] for k in col_order], axis=0) for i in range(2))
    out = dot3(left, right)
    share = out.shape[0] // cols
    for n, ref in enumerate(out_refs):
        ref[...] = out[n * share : (n + 1) * share]


def symbol_kernel(sx_ref, sy_ref, sz_ref, out_ref):
    share_x, share_y = out_ref.shape[0], out_ref.shape[1]
    at_x = lax.axis_index("row") * share_x
    at_y = lax.axis_index("col") * share_y
    place = lax.broadcasted_iota(jnp.int32, (share_y, 1), 0)
    part_y = jnp.zeros((share_y, 1), jnp.float32)
    for j in range(share_y):
        part_y = jnp.where(place == j, sy_ref[at_y + j], part_y)
    yz = part_y + sz_ref[...]
    for i in range(share_x):
        out_ref[i] = 1.0 / (yz + sx_ref[at_x + i])


def z_kernel(*refs, order, fields):
    cols = len(order)
    piece_refs = refs[:cols]
    inverse_ref, t_ref, out_ref, o_ref, sems = refs[cols:]
    me = lax.axis_index("col")
    share_x, share_y, all_z = inverse_ref.shape
    part = piece_refs[0].shape[-1] // fields
    right = tuple(jnp.concatenate([t_ref[i, me ^ k] for k in order], axis=0) for i in range(2))
    inverse = inverse_ref[...]
    copies = []
    for f in range(fields):
        a = jnp.concatenate([r[:, f * part : (f + 1) * part] for r in piece_refs], axis=-1)
        out = dot3(split(a), right)
        o_ref[f] = out.reshape(share_x, share_y, all_z) * inverse
        copies.append(pltpu.make_async_copy(o_ref.at[f], out_ref.at[f], sems.at[f]))
        copies[-1].start()
    for copy in copies:
        copy.wait()


def exchange(pieces, axis, order):
    count = len(order)
    return [
        lax.ppermute(piece, axis, [(i, i ^ k) for i in range(count)]) if k else piece
        for k, piece in zip(order, pieces)
    ]


def fast(species, symbol_x, symbol_y, symbol_z, *, rows, cols):
    fields, all_x, part_y, part_z = species.shape
    all_y, all_z = part_y * rows, part_z * cols
    share_x, share_y = all_x // rows, all_y // cols
    width = fields * part_z
    row_order = [0, *range(rows - 1, 0, -1)]
    col_order = [0, *sorted(range(1, cols), key=lambda k: (k < cols // 2, k))]
    vmem = pl.BlockSpec(memory_space=pltpu.VMEM)
    smem = pl.BlockSpec(memory_space=pltpu.SMEM)
    hbm = pl.BlockSpec(memory_space=pltpu.HBM)
    params = pltpu.CompilerParams(vmem_limit_bytes=VMEM)

    table_x = np.kron(sine_table(all_x), np.eye(part_y, dtype=np.float32))
    table_x = table_x.reshape(rows, share_x * part_y, all_x * part_y)
    table_y = sine_table(all_y).reshape(cols, share_y, rows, part_y)
    table_y = np.einsum("cjry,ab->cajrby", table_y, np.eye(share_x, dtype=np.float32))
    table_y = table_y.reshape(cols, share_x * share_y, rows * share_x * part_y)
    table_z = sine_table(all_z).reshape(cols, part_z, all_z)
    table_x, table_y, table_z = two_terms(table_x), two_terms(table_y), two_terms(table_z)

    piece = jax.ShapeDtypeStruct((share_x * part_y, width), jnp.float32)
    pieces = pl.pallas_call(
        functools.partial(x_kernel, order=row_order),
        out_shape=[piece] * rows,
        in_specs=[hbm, hbm],
        out_specs=[vmem] * rows,
        scratch_shapes=[
            pltpu.VMEM((fields, all_x * part_y, part_z), jnp.float32),
            pltpu.VMEM(table_x.shape, jnp.bfloat16),
            pltpu.SemaphoreType.DMA((fields + 1,)),
        ],
        compiler_params=params,
        name="x_modes",
    )(
        pltpu.with_memory_space_constraint(
            species.reshape(fields, all_x * part_y, part_z), pltpu.HBM
        ),
        pltpu.with_memory_space_constraint(jnp.asarray(table_x), pltpu.HBM),
    )
    pieces = exchange(pieces, "row", row_order)

    block = jax.ShapeDtypeStruct((share_x * share_y, width), jnp.float32)
    line = pltpu.VMEM((rows, share_x * part_y, width), jnp.bfloat16)
    blocks = pl.pallas_call(
        functools.partial(y_kernel, row_order=row_order, col_order=col_order),
        out_shape=[block] * cols,
        in_specs=[vmem] * (rows + 1),
        out_specs=[vmem] * cols,
        scratch_shapes=[line, line],
        compiler_params=params,
        name="y_modes",
    )(*pieces, table_y)
    blocks = exchange(blocks, "col", col_order)

    inverse = pl.pallas_call(
        symbol_kernel,
        out_shape=jax.ShapeDtypeStruct((share_x, share_y, all_z), jnp.float32),
        in_specs=[smem, smem, vmem],
        out_specs=vmem,
        compiler_params=params,
        name="inverse_symbol",
    )(symbol_x, symbol_y, symbol_z[None])
    return pl.pallas_call(
        functools.partial(z_kernel, order=col_order, fields=fields),
        out_shape=jax.ShapeDtypeStruct((fields, share_x, share_y, all_z), jnp.float32),
        in_specs=[vmem] * (cols + 2),
        out_specs=hbm,
        scratch_shapes=[
            pltpu.VMEM((fields, share_x, share_y, all_z), jnp.float32),
            pltpu.SemaphoreType.DMA((fields,)),
        ],
        compiler_params=params,
        name="z_modes",
    )(*blocks, inverse, table_z)


def plain_transform(values, dim):
    table = jnp.asarray(sine_table(values.shape[dim]))
    moved = jnp.tensordot(values, table, axes=([dim], [0]), precision=lax.Precision.HIGHEST)
    return jnp.moveaxis(moved, -1, dim)


def plain(species, symbol_x, symbol_y, symbol_z):
    values = plain_transform(species, 1)
    values = lax.all_to_all(values, "row", split_axis=1, concat_axis=2, tiled=True)
    values = plain_transform(values, 2)
    values = lax.all_to_all(values, "col", split_axis=2, concat_axis=3, tiled=True)
    values = plain_transform(values, 3)
    share_x, share_y = values.shape[1], values.shape[2]
    part_x = lax.dynamic_slice_in_dim(symbol_x, lax.axis_index("row") * share_x, share_x)
    part_y = lax.dynamic_slice_in_dim(symbol_y, lax.axis_index("col") * share_y, share_y)
    return values / (part_x[:, None, None] + part_y[None, :, None] + symbol_z)


def solution(mesh):
    rows, cols = mesh.shape["row"], mesh.shape["col"]

    def on_device(species, symbol_x, symbol_y, symbol_z):
        direct = all(n <= DIRECT and n & (n - 1) == 0 for n in (rows, cols))
        if direct and species.shape[3] * species.shape[0] % LANES == 0:
            return fast(species, symbol_x, symbol_y, symbol_z, rows=rows, cols=cols)
        return plain(species, symbol_x, symbol_y, symbol_z)

    return jax.shard_map(
        on_device,
        mesh=mesh,
        in_specs=(P(None, None, "row", "col"), P(), P(), P()),
        out_specs=P(None, "row", "col", None),
        check_vma=False,
    )
```

```python
import functools

import jax
import jax.numpy as jnp
import numpy as np
from jax import lax
from jax.experimental import pallas as pl
from jax.experimental.pallas import tpu as pltpu
from jax.sharding import PartitionSpec as P


LANES = 128
VMEM = 6 << 20
DIRECT = 16


def sine_table(count):
    rank = np.arange(1, count + 1)
    angle = np.pi / (count + 1) * (np.outer(rank, rank) % (2 * count + 2))
    return (np.sin(angle) * np.sqrt(2.0 / (count + 1))).astype(np.float32)


def two_terms(table):
    high = table.astype(jnp.bfloat16)
    low = (table - high.astype(np.float32)).astype(jnp.bfloat16)
    return np.stack([high, low])


def split(values):
    high = values.astype(jnp.bfloat16)
    low = (values - high.astype(jnp.float32)).astype(jnp.bfloat16)
    return high, low


def dot(left, right):
    return lax.dot_general(
        left, right, (((1,), (0,)), ((), ())), preferred_element_type=jnp.float32
    )


def dot3(left, right):
    return dot(left[0], right[0]) + dot(left[0], right[1]) + dot(left[1], right[0])


def x_kernel(species_ref, table_ref, *refs, order):
    out_refs, (a_ref, t_ref, sems) = refs[: len(order)], refs[len(order) :]
    me = lax.axis_index("row")
    fields = a_ref.shape[0]
    table = pltpu.make_async_copy(table_ref, t_ref, sems.at[fields])
    table.start()
    copies = [
        pltpu.make_async_copy(species_ref.at[f], a_ref.at[f], sems.at[f]) for f in range(fields)
    ]
    for copy in copies:
        copy.start()
    share, all_x = t_ref.shape[1], t_ref.shape[2] // 3
    part_y = a_ref.shape[1] // all_x
    table.wait()
    left = jnp.concatenate([t_ref[me ^ k] for ks in order for k in ks], axis=0)
    left = left.astype(jnp.bfloat16)
    for copy in copies:
        copy.wait()
    for y in range(part_y):
        rows = pl.ds(y, all_x, stride=part_y)
        high, low = split(jnp.concatenate([a_ref[f, rows, :] for f in range(fields)], axis=-1))
        out = dot(left, jnp.concatenate([high, low, high], axis=0))
        n = 0
        for ref, ks in zip(out_refs, order):
            for h in range(len(ks)):
                at = (h * part_y + y) * share
                ref[at : at + share] = out[n * share : (n + 1) * share]
                n += 1


def y_kernel(*refs, row_order, col_order):
    count, cols = len(row_order), len(col_order)
    piece_refs = refs[:count]
    t_ref = refs[count]
    out_refs = refs[count + 1 : count + 1 + cols]
    ch_ref, cl_ref = refs[count + 1 + cols :]
    me_r, me_c = lax.axis_index("row"), lax.axis_index("col")
    size = ch_ref.shape[1]
    for k, ref in zip(row_order, piece_refs):
        high, low = split(ref[ref.shape[0] - size :])
        ch_ref[me_r ^ k] = high
        cl_ref[me_r ^ k] = low
    width = ch_ref.shape[-1]
    right = tuple(r[...].reshape(-1, width) for r in (ch_ref, cl_ref))
    left = tuple(jnp.concatenate([t_ref[i, me_c ^ k] for k in col_order], axis=0) for i in range(2))
    out = dot3(left, right)
    share = out.shape[0] // cols
    for n, ref in enumerate(out_refs):
        ref[...] = out[n * share : (n + 1) * share]


def symbol_kernel(sx_ref, sy_ref, sz_ref, out_ref):
    share_x, share_y = out_ref.shape[0], out_ref.shape[1]
    at_x = lax.axis_index("row") * share_x
    at_y = lax.axis_index("col") * share_y
    place = lax.broadcasted_iota(jnp.int32, (share_y, 1), 0)
    part_y = jnp.zeros((share_y, 1), jnp.float32)
    for j in range(share_y):
        part_y = jnp.where(place == j, sy_ref[at_y + j], part_y)
    yz = part_y + sz_ref[...]
    for i in range(share_x):
        out_ref[i] = 1.0 / (yz + sx_ref[at_x + i])


def z_kernel(*refs, order, fields):
    cols = len(order)
    piece_refs = refs[:cols]
    inverse_ref, t_ref, out_ref, o_ref, sems = refs[cols:]
    me = lax.axis_index("col")
    share_x, share_y, all_z = inverse_ref.shape
    part = piece_refs[0].shape[-1] // fields
    right = tuple(jnp.concatenate([t_ref[i, me ^ k] for k in order], axis=0) for i in range(2))
    inverse = inverse_ref[...]
    copies = []
    for f in range(fields):
        a = jnp.concatenate([r[:, f * part : (f + 1) * part] for r in piece_refs], axis=-1)
        out = dot3(split(a), right)
        o_ref[f] = out.reshape(share_x, share_y, all_z) * inverse
        copies.append(pltpu.make_async_copy(o_ref.at[f], out_ref.at[f], sems.at[f]))
        copies[-1].start()
    for copy in copies:
        copy.wait()


def exchange(pieces, axis, order):
    count = len(order)
    return [
        lax.ppermute(piece, axis, [(i, i ^ k) for i in range(count)]) if k else piece
        for k, piece in zip(order, pieces)
    ]


def exchange_rows(pieces, order, rows):
    here = {0: pieces[0]}
    size = pieces[0].shape[0]

    def send(piece, k):
        return lax.ppermute(piece, "row", [(i, i ^ k) for i in range(rows)])

    for ks, piece in zip(order[1:], pieces[1:]):
        here[ks[-1]] = send(piece, ks[-1])
    for ks in order[1:]:
        if len(ks) == 2:
            here[ks[0]] = send(here[ks[-1]][:size], 1)
    return here


def fast(species, symbol_x, symbol_y, symbol_z, *, rows, cols):
    fields, all_x, part_y, part_z = species.shape
    all_y, all_z = part_y * rows, part_z * cols
    share_x, share_y = all_x // rows, all_y // cols
    width = fields * part_z
    row_order = [(0,), *((k - 1, k) for k in range(rows - 1, 1, -2)), (1,)]
    col_order = [0, *sorted(range(1, cols), key=lambda k: (k < cols // 2, k))]
    vmem = pl.BlockSpec(memory_space=pltpu.VMEM)
    smem = pl.BlockSpec(memory_space=pltpu.SMEM)
    hbm = pl.BlockSpec(memory_space=pltpu.HBM)
    params = pltpu.CompilerParams(vmem_limit_bytes=VMEM)

    high, low = two_terms(sine_table(all_x)).astype(np.float32)
    table_x = np.concatenate([high, high, low], axis=1).reshape(rows, share_x, 3 * all_x)
    table_y = sine_table(all_y).reshape(cols, share_y, rows, part_y)
    table_y = np.einsum("cjry,ab->cajryb", table_y, np.eye(share_x, dtype=np.float32))
    table_y = table_y.reshape(cols, share_x * share_y, rows * share_x * part_y)
    table_z = sine_table(all_z).reshape(cols, part_z, all_z)
    table_y, table_z = two_terms(table_y), two_terms(table_z)

    pieces = pl.pallas_call(
        functools.partial(x_kernel, order=row_order),
        out_shape=[
            jax.ShapeDtypeStruct((len(ks) * share_x * part_y, width), jnp.float32)
            for ks in row_order
        ],
        in_specs=[hbm, hbm],
        out_specs=[vmem] * len(row_order),
        scratch_shapes=[
            pltpu.VMEM((fields, all_x * part_y, part_z), jnp.float32),
            pltpu.VMEM(table_x.shape, jnp.float32),
            pltpu.SemaphoreType.DMA((fields + 1,)),
        ],
        compiler_params=params,
        name="x_modes",
    )(
        pltpu.with_memory_space_constraint(
            species.reshape(fields, all_x * part_y, part_z), pltpu.HBM
        ),
        pltpu.with_memory_space_constraint(jnp.asarray(table_x), pltpu.HBM),
    )
    pieces = exchange_rows(pieces, row_order, rows)

    block = jax.ShapeDtypeStruct((share_x * share_y, width), jnp.float32)
    line = pltpu.VMEM((rows, share_x * part_y, width), jnp.bfloat16)
    blocks = pl.pallas_call(
        functools.partial(y_kernel, row_order=list(pieces), col_order=col_order),
        out_shape=[block] * cols,
        in_specs=[vmem] * (rows + 1),
        out_specs=[vmem] * cols,
        scratch_shapes=[line, line],
        compiler_params=params,
        name="y_modes",
    )(*pieces.values(), table_y)
    blocks = exchange(blocks, "col", col_order)

    inverse = pl.pallas_call(
        symbol_kernel,
        out_shape=jax.ShapeDtypeStruct((share_x, share_y, all_z), jnp.float32),
        in_specs=[smem, smem, vmem],
        out_specs=vmem,
        compiler_params=params,
        name="inverse_symbol",
    )(symbol_x, symbol_y, symbol_z[None])
    return pl.pallas_call(
        functools.partial(z_kernel, order=col_order, fields=fields),
        out_shape=jax.ShapeDtypeStruct((fields, share_x, share_y, all_z), jnp.float32),
        in_specs=[vmem] * (cols + 2),
        out_specs=hbm,
        scratch_shapes=[
            pltpu.VMEM((fields, share_x, share_y, all_z), jnp.float32),
            pltpu.SemaphoreType.DMA((fields,)),
        ],
        compiler_params=params,
        name="z_modes",
    )(*blocks, inverse, table_z)


def plain_transform(values, dim):
    table = jnp.asarray(sine_table(values.shape[dim]))
    moved = jnp.tensordot(values, table, axes=([dim], [0]), precision=lax.Precision.HIGHEST)
    return jnp.moveaxis(moved, -1, dim)


def plain(species, symbol_x, symbol_y, symbol_z):
    values = plain_transform(species, 1)
    values = lax.all_to_all(values, "row", split_axis=1, concat_axis=2, tiled=True)
    values = plain_transform(values, 2)
    values = lax.all_to_all(values, "col", split_axis=2, concat_axis=3, tiled=True)
    values = plain_transform(values, 3)
    share_x, share_y = values.shape[1], values.shape[2]
    part_x = lax.dynamic_slice_in_dim(symbol_x, lax.axis_index("row") * share_x, share_x)
    part_y = lax.dynamic_slice_in_dim(symbol_y, lax.axis_index("col") * share_y, share_y)
    return values / (part_x[:, None, None] + part_y[None, :, None] + symbol_z)


def solution(mesh):
    rows, cols = mesh.shape["row"], mesh.shape["col"]

    def on_device(species, symbol_x, symbol_y, symbol_z):
        direct = all(n <= DIRECT and n & (n - 1) == 0 for n in (rows, cols))
        if direct and species.shape[3] * species.shape[0] % LANES == 0:
            return fast(species, symbol_x, symbol_y, symbol_z, rows=rows, cols=cols)
        return plain(species, symbol_x, symbol_y, symbol_z)

    return jax.shard_map(
        on_device,
        mesh=mesh,
        in_specs=(P(None, None, "row", "col"), P(), P(), P()),
        out_specs=P(None, "row", "col", None),
        check_vma=False,
    )
```

```python
import functools

import jax
import jax.numpy as jnp
import numpy as np
from jax import lax
from jax.experimental import pallas as pl
from jax.experimental.pallas import tpu as pltpu
from jax.sharding import PartitionSpec as P


LANES = 128
VMEM = 6 << 20
DIRECT = 16


def sine_table(count):
    rank = np.arange(1, count + 1)
    angle = np.pi / (count + 1) * (np.outer(rank, rank) % (2 * count + 2))
    return (np.sin(angle) * np.sqrt(2.0 / (count + 1))).astype(np.float32)


def two_terms(table):
    high = table.astype(jnp.bfloat16)
    low = (table - high.astype(np.float32)).astype(jnp.bfloat16)
    return np.stack([high, low])


def split(values):
    high = values.astype(jnp.bfloat16)
    low = (values - high.astype(jnp.float32)).astype(jnp.bfloat16)
    return high, low


def dot(left, right):
    return lax.dot_general(
        left, right, (((1,), (0,)), ((), ())), preferred_element_type=jnp.float32
    )


def dot3(left, right):
    return dot(left[0], right[0]) + dot(left[0], right[1]) + dot(left[1], right[0])


def x_kernel(species_ref, table_ref, *refs, order):
    out_refs, (a_ref, t_ref, sems) = refs[: len(order)], refs[len(order) :]
    me = lax.axis_index("row")
    fields = a_ref.shape[0]
    table = pltpu.make_async_copy(table_ref, t_ref, sems.at[fields])
    table.start()
    copies = [
        pltpu.make_async_copy(species_ref.at[f], a_ref.at[f], sems.at[f]) for f in range(fields)
    ]
    for copy in copies:
        copy.start()
    share, all_x = t_ref.shape[1], t_ref.shape[2] // 3
    part_y = a_ref.shape[1] // all_x
    table.wait()
    left = jnp.concatenate([t_ref[me ^ k] for ks in order for k in ks], axis=0)
    left = left.astype(jnp.bfloat16)
    for copy in copies:
        copy.wait()
    for y in range(part_y):
        rows = pl.ds(y, all_x, stride=part_y)
        high, low = split(jnp.concatenate([a_ref[f, rows, :] for f in range(fields)], axis=-1))
        out = dot(left, jnp.concatenate([high, low, high], axis=0))
        n = 0
        for ref, ks in zip(out_refs, order):
            for h in range(len(ks)):
                at = (h * part_y + y) * share
                ref[at : at + share] = out[n * share : (n + 1) * share]
                n += 1


def y_kernel(*refs, row_order, col_order):
    count, cols = len(row_order), len(col_order)
    piece_refs = refs[:count]
    t_ref = refs[count]
    out_refs = refs[count + 1 : count + 1 + cols]
    ch_ref, cl_ref = refs[count + 1 + cols :]
    me_r, me_c = lax.axis_index("row"), lax.axis_index("col")
    size = ch_ref.shape[1]
    for k, ref in zip(row_order, piece_refs):
        high, low = split(ref[ref.shape[0] - size :])
        ch_ref[me_r ^ k] = high
        cl_ref[me_r ^ k] = low
    width = ch_ref.shape[-1]
    right = tuple(r[...].reshape(-1, width) for r in (ch_ref, cl_ref))
    left = tuple(jnp.concatenate([t_ref[i, me_c ^ k] for k in col_order], axis=0) for i in range(2))
    out = dot3(left, right)
    share = out.shape[0] // cols
    for n, ref in enumerate(out_refs):
        ref[...] = out[n * share : (n + 1) * share]


def symbol_kernel(sx_ref, sy_ref, sz_ref, out_ref):
    share_x, share_y = out_ref.shape[0], out_ref.shape[1]
    at_x = lax.axis_index("row") * share_x
    at_y = lax.axis_index("col") * share_y
    place = lax.broadcasted_iota(jnp.int32, (share_y, 1), 0)
    part_y = jnp.zeros((share_y, 1), jnp.float32)
    for j in range(share_y):
        part_y = jnp.where(place == j, sy_ref[at_y + j], part_y)
    yz = part_y + sz_ref[...]
    for i in range(share_x):
        out_ref[i] = 1.0 / (yz + sx_ref[at_x + i])


def z_kernel(*refs, order, fields):
    cols = len(order)
    piece_refs = refs[:cols]
    inverse_ref, t_ref, out_ref, o_ref, sems = refs[cols:]
    me = lax.axis_index("col")
    share_x, share_y, all_z = inverse_ref.shape
    part = piece_refs[0].shape[-1] // fields
    right = tuple(jnp.concatenate([t_ref[i, me ^ k] for k in order], axis=0) for i in range(2))
    inverse = inverse_ref[...]
    copies = []
    for f in range(fields):
        a = jnp.concatenate([r[:, f * part : (f + 1) * part] for r in piece_refs], axis=-1)
        out = dot3(split(a), right)
        o_ref[f] = out.reshape(share_x, share_y, all_z) * inverse
        copies.append(pltpu.make_async_copy(o_ref.at[f], out_ref.at[f], sems.at[f]))
        copies[-1].start()
    for copy in copies:
        copy.wait()


def exchange(pieces, axis, order):
    count = len(order)
    return [
        lax.ppermute(piece, axis, [(i, i ^ k) for i in range(count)]) if k else piece
        for k, piece in zip(order, pieces)
    ]


def exchange_rows(pieces, order, rows):
    here = {0: pieces[0]}
    size = pieces[0].shape[0]

    def send(piece, k):
        return lax.ppermute(piece, "row", [(i, i ^ k) for i in range(rows)])

    for ks, piece in zip(order[1:], pieces[1:]):
        here[ks[-1]] = send(piece, ks[-1])
    for ks in order[1:]:
        if len(ks) == 2:
            here[ks[0]] = send(here[ks[-1]][:size], 1)
    return here


def fast(species, symbol_x, symbol_y, symbol_z, *, rows, cols):
    fields, all_x, part_y, part_z = species.shape
    all_y, all_z = part_y * rows, part_z * cols
    share_x, share_y = all_x // rows, all_y // cols
    width = fields * part_z
    row_order = [(0,), *((k ^ 1, k) for k in range(5, rows, 2))]
    row_order += [(k,) for k in (3, 1, 2) if k < rows]
    col_order = [0, *sorted(range(1, cols), key=lambda k: (k < cols // 2, k))]
    vmem = pl.BlockSpec(memory_space=pltpu.VMEM)
    smem = pl.BlockSpec(memory_space=pltpu.SMEM)
    hbm = pl.BlockSpec(memory_space=pltpu.HBM)
    params = pltpu.CompilerParams(vmem_limit_bytes=VMEM)

    high, low = two_terms(sine_table(all_x)).astype(np.float32)
    table_x = np.concatenate([high, high, low], axis=1).reshape(rows, share_x, 3 * all_x)
    table_y = sine_table(all_y).reshape(cols, share_y, rows, part_y)
    table_y = np.einsum("cjry,ab->cajryb", table_y, np.eye(share_x, dtype=np.float32))
    table_y = table_y.reshape(cols, share_x * share_y, rows * share_x * part_y)
    table_z = sine_table(all_z).reshape(cols, part_z, all_z)
    table_y, table_z = two_terms(table_y), two_terms(table_z)

    pieces = pl.pallas_call(
        functools.partial(x_kernel, order=row_order),
        out_shape=[
            jax.ShapeDtypeStruct((len(ks) * share_x * part_y, width), jnp.float32)
            for ks in row_order
        ],
        in_specs=[hbm, hbm],
        out_specs=[vmem] * len(row_order),
        scratch_shapes=[
            pltpu.VMEM((fields, all_x * part_y, part_z), jnp.float32),
            pltpu.VMEM(table_x.shape, jnp.float32),
            pltpu.SemaphoreType.DMA((fields + 1,)),
        ],
        compiler_params=params,
        name="x_modes",
    )(
        pltpu.with_memory_space_constraint(
            species.reshape(fields, all_x * part_y, part_z), pltpu.HBM
        ),
        pltpu.with_memory_space_constraint(jnp.asarray(table_x), pltpu.HBM),
    )
    pieces = exchange_rows(pieces, row_order, rows)

    block = jax.ShapeDtypeStruct((share_x * share_y, width), jnp.float32)
    line = pltpu.VMEM((rows, share_x * part_y, width), jnp.bfloat16)
    blocks = pl.pallas_call(
        functools.partial(y_kernel, row_order=list(pieces), col_order=col_order),
        out_shape=[block] * cols,
        in_specs=[vmem] * (rows + 1),
        out_specs=[vmem] * cols,
        scratch_shapes=[line, line],
        compiler_params=params,
        name="y_modes",
    )(*pieces.values(), table_y)
    blocks = exchange(blocks, "col", col_order)

    inverse = pl.pallas_call(
        symbol_kernel,
        out_shape=jax.ShapeDtypeStruct((share_x, share_y, all_z), jnp.float32),
        in_specs=[smem, smem, vmem],
        out_specs=vmem,
        compiler_params=params,
        name="inverse_symbol",
    )(symbol_x, symbol_y, symbol_z[None])
    return pl.pallas_call(
        functools.partial(z_kernel, order=col_order, fields=fields),
        out_shape=jax.ShapeDtypeStruct((fields, share_x, share_y, all_z), jnp.float32),
        in_specs=[vmem] * (cols + 2),
        out_specs=hbm,
        scratch_shapes=[
            pltpu.VMEM((fields, share_x, share_y, all_z), jnp.float32),
            pltpu.SemaphoreType.DMA((fields,)),
        ],
        compiler_params=params,
        name="z_modes",
    )(*blocks, inverse, table_z)


def plain_transform(values, dim):
    table = jnp.asarray(sine_table(values.shape[dim]))
    moved = jnp.tensordot(values, table, axes=([dim], [0]), precision=lax.Precision.HIGHEST)
    return jnp.moveaxis(moved, -1, dim)


def plain(species, symbol_x, symbol_y, symbol_z):
    values = plain_transform(species, 1)
    values = lax.all_to_all(values, "row", split_axis=1, concat_axis=2, tiled=True)
    values = plain_transform(values, 2)
    values = lax.all_to_all(values, "col", split_axis=2, concat_axis=3, tiled=True)
    values = plain_transform(values, 3)
    share_x, share_y = values.shape[1], values.shape[2]
    part_x = lax.dynamic_slice_in_dim(symbol_x, lax.axis_index("row") * share_x, share_x)
    part_y = lax.dynamic_slice_in_dim(symbol_y, lax.axis_index("col") * share_y, share_y)
    return values / (part_x[:, None, None] + part_y[None, :, None] + symbol_z)


def solution(mesh):
    rows, cols = mesh.shape["row"], mesh.shape["col"]

    def on_device(species, symbol_x, symbol_y, symbol_z):
        direct = all(n <= DIRECT and n & (n - 1) == 0 for n in (rows, cols))
        if direct and species.shape[3] * species.shape[0] % LANES == 0:
            return fast(species, symbol_x, symbol_y, symbol_z, rows=rows, cols=cols)
        return plain(species, symbol_x, symbol_y, symbol_z)

    return jax.shard_map(
        on_device,
        mesh=mesh,
        in_specs=(P(None, None, "row", "col"), P(), P(), P()),
        out_specs=P(None, "row", "col", None),
        check_vma=False,
    )
```

```python
import functools

import jax
import jax.numpy as jnp
import numpy as np
from jax import lax
from jax.experimental import pallas as pl
from jax.experimental.pallas import tpu as pltpu
from jax.sharding import PartitionSpec as P


LANES = 128
VMEM = 6 << 20
DIRECT = 16


def sine_table(count):
    rank = np.arange(1, count + 1)
    angle = np.pi / (count + 1) * (np.outer(rank, rank) % (2 * count + 2))
    return (np.sin(angle) * np.sqrt(2.0 / (count + 1))).astype(np.float32)


def two_terms(table):
    high = table.astype(jnp.bfloat16)
    low = (table - high.astype(np.float32)).astype(jnp.bfloat16)
    return np.stack([high, low])


def split(values):
    high = values.astype(jnp.bfloat16)
    low = (values - high.astype(jnp.float32)).astype(jnp.bfloat16)
    return high, low


def dot(left, right):
    return lax.dot_general(
        left, right, (((1,), (0,)), ((), ())), preferred_element_type=jnp.float32
    )


def dot3(left, right):
    return dot(left[0], right[0]) + dot(left[0], right[1]) + dot(left[1], right[0])


def round_trips(cols):
    gray = [i ^ (i >> 1) for i in range(cols)]
    cycles = gray, list(range(cols))
    return [
        tuple(tuple(c[(c.index(i) + n) % cols] for i in range(cols)) for c in cycles)
        for n in range(cols)
    ]


def look(table, at):
    found = jnp.int32(table[0])
    for i in range(1, len(table)):
        found = jnp.where(at == i, jnp.int32(table[i]), found)
    return found


def target(step, me_r, me_c):
    return jnp.where(me_r % 2 == 0, look(step[0], me_c), look(step[1], me_c))


def source(step, me_r, me_c):
    back = [tuple(table.index(i) for i in range(len(table))) for table in step]
    return target(back, me_r, me_c)


def x_kernel(species_ref, table_ref, *refs, order):
    out_refs, (a_ref, t_ref, sems) = refs[: len(order)], refs[len(order) :]
    me = lax.axis_index("row")
    fields = a_ref.shape[0]
    table = pltpu.make_async_copy(table_ref, t_ref, sems.at[fields])
    table.start()
    copies = [
        pltpu.make_async_copy(species_ref.at[f], a_ref.at[f], sems.at[f]) for f in range(fields)
    ]
    for copy in copies:
        copy.start()
    share, all_x = t_ref.shape[1], t_ref.shape[2] // 3
    part_y = a_ref.shape[1] // all_x
    table.wait()
    left = jnp.concatenate([t_ref[me ^ k] for ks in order for k in ks], axis=0)
    left = left.astype(jnp.bfloat16)
    for copy in copies:
        copy.wait()
    for y in range(part_y):
        rows = pl.ds(y, all_x, stride=part_y)
        high, low = split(jnp.concatenate([a_ref[f, rows, :] for f in range(fields)], axis=-1))
        out = dot(left, jnp.concatenate([high, low, high], axis=0))
        n = 0
        for ref, ks in zip(out_refs, order):
            for h in range(len(ks)):
                at = (h * part_y + y) * share
                ref[at : at + share] = out[n * share : (n + 1) * share]
                n += 1


def y_kernel(*refs, row_order, col_steps):
    count, cols = len(row_order), len(col_steps)
    piece_refs = refs[:count]
    t_ref = refs[count]
    out_refs = refs[count + 1 : count + 1 + cols]
    ch_ref, cl_ref = refs[count + 1 + cols :]
    me_r, me_c = lax.axis_index("row"), lax.axis_index("col")
    size = ch_ref.shape[1]
    for k, ref in zip(row_order, piece_refs):
        high, low = split(ref[ref.shape[0] - size :])
        ch_ref[me_r ^ k] = high
        cl_ref[me_r ^ k] = low
    width = ch_ref.shape[-1]
    right = tuple(r[...].reshape(-1, width) for r in (ch_ref, cl_ref))
    to = [target(step, me_r, me_c) for step in col_steps]
    left = tuple(jnp.concatenate([t_ref[i, c] for c in to], axis=0) for i in range(2))
    out = dot3(left, right)
    share = out.shape[0] // cols
    for n, ref in enumerate(out_refs):
        ref[...] = out[n * share : (n + 1) * share]


def symbol_kernel(sx_ref, sy_ref, sz_ref, out_ref):
    share_x, share_y = out_ref.shape[0], out_ref.shape[1]
    at_x = lax.axis_index("row") * share_x
    at_y = lax.axis_index("col") * share_y
    place = lax.broadcasted_iota(jnp.int32, (share_y, 1), 0)
    part_y = jnp.zeros((share_y, 1), jnp.float32)
    for j in range(share_y):
        part_y = jnp.where(place == j, sy_ref[at_y + j], part_y)
    yz = part_y + sz_ref[...]
    for i in range(share_x):
        out_ref[i] = 1.0 / (yz + sx_ref[at_x + i])


def z_kernel(*refs, col_steps, fields):
    cols = len(col_steps)
    piece_refs = refs[:cols]
    inverse_ref, t_ref, out_ref, o_ref, sems = refs[cols:]
    me_r, me_c = lax.axis_index("row"), lax.axis_index("col")
    share_x, share_y, all_z = inverse_ref.shape
    part = piece_refs[0].shape[-1] // fields
    by = [source(step, me_r, me_c) for step in col_steps]
    right = tuple(jnp.concatenate([t_ref[i, c] for c in by], axis=0) for i in range(2))
    inverse = inverse_ref[...]
    copies = []
    for f in range(fields):
        a = jnp.concatenate([r[:, f * part : (f + 1) * part] for r in piece_refs], axis=-1)
        out = dot3(split(a), right)
        o_ref[f] = out.reshape(share_x, share_y, all_z) * inverse
        copies.append(pltpu.make_async_copy(o_ref.at[f], out_ref.at[f], sems.at[f]))
        copies[-1].start()
    for copy in copies:
        copy.wait()


def exchange_cols(blocks, steps, rows, cols):
    got = [blocks[0]]
    for step, block in zip(steps[1:], blocks[1:]):
        pairs = [(r * cols + c, r * cols + step[r % 2][c]) for r in range(rows) for c in range(cols)]
        got.append(lax.ppermute(block, ("row", "col"), pairs))
    return got


def exchange_rows(pieces, order, rows):
    here = {0: pieces[0]}
    size = pieces[0].shape[0]

    def send(piece, k):
        return lax.ppermute(piece, "row", [(i, i ^ k) for i in range(rows)])

    for ks, piece in zip(order[1:], pieces[1:]):
        here[ks[-1]] = send(piece, ks[-1])
    for ks in order[1:]:
        if len(ks) == 2:
            here[ks[0]] = send(here[ks[-1]][:size], 1)
    return here


def fast(species, symbol_x, symbol_y, symbol_z, *, rows, cols):
    fields, all_x, part_y, part_z = species.shape
    all_y, all_z = part_y * rows, part_z * cols
    share_x, share_y = all_x // rows, all_y // cols
    width = fields * part_z
    row_order = [(0,), *((k ^ 1, k) for k in range(5, rows, 2))]
    row_order += [(k,) for k in (3, 1, 2) if k < rows]
    col_steps = round_trips(cols)
    vmem = pl.BlockSpec(memory_space=pltpu.VMEM)
    smem = pl.BlockSpec(memory_space=pltpu.SMEM)
    hbm = pl.BlockSpec(memory_space=pltpu.HBM)
    params = pltpu.CompilerParams(vmem_limit_bytes=VMEM)

    high, low = two_terms(sine_table(all_x)).astype(np.float32)
    table_x = np.concatenate([high, high, low], axis=1).reshape(rows, share_x, 3 * all_x)
    table_y = sine_table(all_y).reshape(cols, share_y, rows, part_y)
    table_y = np.einsum("cjry,ab->cajryb", table_y, np.eye(share_x, dtype=np.float32))
    table_y = table_y.reshape(cols, share_x * share_y, rows * share_x * part_y)
    table_z = sine_table(all_z).reshape(cols, part_z, all_z)
    table_y, table_z = two_terms(table_y), two_terms(table_z)

    pieces = pl.pallas_call(
        functools.partial(x_kernel, order=row_order),
        out_shape=[
            jax.ShapeDtypeStruct((len(ks) * share_x * part_y, width), jnp.float32)
            for ks in row_order
        ],
        in_specs=[hbm, hbm],
        out_specs=[vmem] * len(row_order),
        scratch_shapes=[
            pltpu.VMEM((fields, all_x * part_y, part_z), jnp.float32),
            pltpu.VMEM(table_x.shape, jnp.float32),
            pltpu.SemaphoreType.DMA((fields + 1,)),
        ],
        compiler_params=params,
        name="x_modes",
    )(
        pltpu.with_memory_space_constraint(
            species.reshape(fields, all_x * part_y, part_z), pltpu.HBM
        ),
        pltpu.with_memory_space_constraint(jnp.asarray(table_x), pltpu.HBM),
    )
    pieces = exchange_rows(pieces, row_order, rows)

    block = jax.ShapeDtypeStruct((share_x * share_y, width), jnp.float32)
    line = pltpu.VMEM((rows, share_x * part_y, width), jnp.bfloat16)
    blocks = pl.pallas_call(
        functools.partial(y_kernel, row_order=list(pieces), col_steps=col_steps),
        out_shape=[block] * cols,
        in_specs=[vmem] * (rows + 1),
        out_specs=[vmem] * cols,
        scratch_shapes=[line, line],
        compiler_params=params,
        name="y_modes",
    )(*pieces.values(), table_y)
    blocks = exchange_cols(blocks, col_steps, rows, cols)

    inverse = pl.pallas_call(
        symbol_kernel,
        out_shape=jax.ShapeDtypeStruct((share_x, share_y, all_z), jnp.float32),
        in_specs=[smem, smem, vmem],
        out_specs=vmem,
        compiler_params=params,
        name="inverse_symbol",
    )(symbol_x, symbol_y, symbol_z[None])
    return pl.pallas_call(
        functools.partial(z_kernel, col_steps=col_steps, fields=fields),
        out_shape=jax.ShapeDtypeStruct((fields, share_x, share_y, all_z), jnp.float32),
        in_specs=[vmem] * (cols + 2),
        out_specs=hbm,
        scratch_shapes=[
            pltpu.VMEM((fields, share_x, share_y, all_z), jnp.float32),
            pltpu.SemaphoreType.DMA((fields,)),
        ],
        compiler_params=params,
        name="z_modes",
    )(*blocks, inverse, table_z)


def plain_transform(values, dim):
    table = jnp.asarray(sine_table(values.shape[dim]))
    moved = jnp.tensordot(values, table, axes=([dim], [0]), precision=lax.Precision.HIGHEST)
    return jnp.moveaxis(moved, -1, dim)


def plain(species, symbol_x, symbol_y, symbol_z):
    values = plain_transform(species, 1)
    values = lax.all_to_all(values, "row", split_axis=1, concat_axis=2, tiled=True)
    values = plain_transform(values, 2)
    values = lax.all_to_all(values, "col", split_axis=2, concat_axis=3, tiled=True)
    values = plain_transform(values, 3)
    share_x, share_y = values.shape[1], values.shape[2]
    part_x = lax.dynamic_slice_in_dim(symbol_x, lax.axis_index("row") * share_x, share_x)
    part_y = lax.dynamic_slice_in_dim(symbol_y, lax.axis_index("col") * share_y, share_y)
    return values / (part_x[:, None, None] + part_y[None, :, None] + symbol_z)


def solution(mesh):
    rows, cols = mesh.shape["row"], mesh.shape["col"]

    def on_device(species, symbol_x, symbol_y, symbol_z):
        direct = all(n <= DIRECT and n & (n - 1) == 0 for n in (rows, cols))
        if direct and species.shape[3] * species.shape[0] % LANES == 0:
            return fast(species, symbol_x, symbol_y, symbol_z, rows=rows, cols=cols)
        return plain(species, symbol_x, symbol_y, symbol_z)

    return jax.shard_map(
        on_device,
        mesh=mesh,
        in_specs=(P(None, None, "row", "col"), P(), P(), P()),
        out_specs=P(None, "row", "col", None),
        check_vma=False,
    )
```

```python
import functools

import jax
import jax.numpy as jnp
import numpy as np
from jax import lax
from jax.experimental import pallas as pl
from jax.experimental.pallas import tpu as pltpu
from jax.sharding import PartitionSpec as P


LANES = 128
VMEM = 6 << 20
DIRECT = 16


def sine_table(count):
    rank = np.arange(1, count + 1)
    angle = np.pi / (count + 1) * (np.outer(rank, rank) % (2 * count + 2))
    return (np.sin(angle) * np.sqrt(2.0 / (count + 1))).astype(np.float32)


def two_terms(table):
    high = table.astype(jnp.bfloat16)
    low = (table - high.astype(np.float32)).astype(jnp.bfloat16)
    return np.stack([high, low])


def split(values):
    high = values.astype(jnp.bfloat16)
    low = (values - high.astype(jnp.float32)).astype(jnp.bfloat16)
    return high, low


def dot(left, right):
    return lax.dot_general(
        left, right, (((1,), (0,)), ((), ())), preferred_element_type=jnp.float32
    )


def dot3(left, right):
    return dot(left[0], right[0]) + dot(left[0], right[1]) + dot(left[1], right[0])


def round_trips(cols):
    gray = [i ^ (i >> 1) for i in range(cols)]
    cycles = gray, list(range(cols))
    return [
        tuple(tuple(c[(c.index(i) + n) % cols] for i in range(cols)) for c in cycles)
        for n in range(cols)
    ]


def look(table, at):
    found = jnp.int32(table[0])
    for i in range(1, len(table)):
        found = jnp.where(at == i, jnp.int32(table[i]), found)
    return found


def target(step, me_r, me_c):
    return jnp.where(me_r % 2 == 0, look(step[0], me_c), look(step[1], me_c))


def source(step, me_r, me_c):
    back = [tuple(table.index(i) for i in range(len(table))) for table in step]
    return target(back, me_r, me_c)


def x_kernel(species_ref, table_ref, *refs, order):
    out_refs, (a_ref, t_ref, sems) = refs[: len(order)], refs[len(order) :]
    me = lax.axis_index("row")
    fields = a_ref.shape[0]
    table = pltpu.make_async_copy(table_ref, t_ref, sems.at[fields])
    table.start()
    copies = [
        pltpu.make_async_copy(species_ref.at[f], a_ref.at[f], sems.at[f]) for f in range(fields)
    ]
    for copy in copies:
        copy.start()
    share, all_x = t_ref.shape[1], t_ref.shape[2] // 3
    part_y = a_ref.shape[1] // all_x
    table.wait()
    left = jnp.concatenate([t_ref[me ^ k] for ks in order for k in ks], axis=0)
    left = left.astype(jnp.bfloat16)
    for copy in copies:
        copy.wait()
    for y in range(part_y):
        rows = pl.ds(y, all_x, stride=part_y)
        high, low = split(jnp.concatenate([a_ref[f, rows, :] for f in range(fields)], axis=-1))
        out = dot(left, jnp.concatenate([high, low, high], axis=0))
        n = 0
        for ref, ks in zip(out_refs, order):
            for h in range(len(ks)):
                at = (h * part_y + y) * share
                ref[at : at + share] = out[n * share : (n + 1) * share]
                n += 1


def y_kernel(*refs, row_order, col_steps):
    count, cols = len(row_order), len(col_steps)
    piece_refs = refs[:count]
    t_ref = refs[count]
    out_refs = refs[count + 1 : count + 1 + cols]
    ch_ref, cl_ref = refs[count + 1 + cols :]
    me_r, me_c = lax.axis_index("row"), lax.axis_index("col")
    size = ch_ref.shape[1]
    for k, ref in zip(row_order, piece_refs):
        high, low = split(ref[ref.shape[0] - size :])
        ch_ref[me_r ^ k] = high
        cl_ref[me_r ^ k] = low
    width = ch_ref.shape[-1]
    right = tuple(r[...].reshape(-1, width) for r in (ch_ref, cl_ref))
    to = [target(step, me_r, me_c) for step in col_steps]
    left = tuple(jnp.concatenate([t_ref[i, c] for c in to], axis=0) for i in range(2))
    out = dot3(left, right)
    share = out.shape[0] // cols
    for n, ref in enumerate(out_refs):
        ref[...] = out[n * share : (n + 1) * share]


def symbol_kernel(sx_ref, sy_ref, sz_ref, out_ref):
    share_x, share_y = out_ref.shape[0], out_ref.shape[1]
    at_x = lax.axis_index("row") * share_x
    at_y = lax.axis_index("col") * share_y
    place = lax.broadcasted_iota(jnp.int32, (share_y, 1), 0)
    part_y = jnp.zeros((share_y, 1), jnp.float32)
    for j in range(share_y):
        part_y = jnp.where(place == j, sy_ref[at_y + j], part_y)
    yz = part_y + sz_ref[...]
    for i in range(share_x):
        out_ref[i] = 1.0 / (yz + sx_ref[at_x + i])


def z_kernel(*refs, col_steps, fields):
    cols = len(col_steps)
    piece_refs = refs[:cols]
    inverse_ref, t_ref, out_ref, o_ref, sems = refs[cols:]
    me_r, me_c = lax.axis_index("row"), lax.axis_index("col")
    share_x, share_y, all_z = inverse_ref.shape
    part = piece_refs[0].shape[-1] // fields
    by = [source(step, me_r, me_c) for step in col_steps]
    right = tuple(jnp.concatenate([t_ref[i, c] for c in by], axis=0) for i in range(2))
    inverse = inverse_ref[...]
    copies = []
    step = 2 - fields % 2
    for f in range(0, fields, step):
        a = jnp.concatenate(
            [
                jnp.concatenate([r[:, g * part : (g + 1) * part] for r in piece_refs], axis=-1)
                for g in range(f, f + step)
            ],
            axis=0,
        )
        here = pl.ds(f, step)
        o_ref[here] = dot3(split(a), right).reshape(step, share_x, share_y, all_z) * inverse
        copies.append(pltpu.make_async_copy(o_ref.at[here], out_ref.at[here], sems.at[f]))
        copies[-1].start()
    for copy in copies:
        copy.wait()


def exchange_cols(blocks, steps, rows, cols):
    got = [blocks[0]]
    for step, block in zip(steps[1:], blocks[1:]):
        pairs = [(r * cols + c, r * cols + step[r % 2][c]) for r in range(rows) for c in range(cols)]
        got.append(lax.ppermute(block, ("row", "col"), pairs))
    return got


def exchange_rows(pieces, order, rows):
    here = {0: pieces[0]}
    size = pieces[0].shape[0]

    def send(piece, k):
        return lax.ppermute(piece, "row", [(i, i ^ k) for i in range(rows)])

    for ks, piece in zip(order[1:], pieces[1:]):
        here[ks[-1]] = send(piece, ks[-1])
    for ks in order[1:]:
        if len(ks) == 2:
            here[ks[0]] = send(here[ks[-1]][:size], 1)
    return here


def fast(species, symbol_x, symbol_y, symbol_z, *, rows, cols):
    fields, all_x, part_y, part_z = species.shape
    all_y, all_z = part_y * rows, part_z * cols
    share_x, share_y = all_x // rows, all_y // cols
    width = fields * part_z
    row_order = [(0,), *((k ^ 1, k) for k in range(5, rows, 2))]
    row_order += [(k,) for k in (3, 1, 2) if k < rows]
    col_steps = round_trips(cols)
    vmem = pl.BlockSpec(memory_space=pltpu.VMEM)
    smem = pl.BlockSpec(memory_space=pltpu.SMEM)
    hbm = pl.BlockSpec(memory_space=pltpu.HBM)
    params = pltpu.CompilerParams(vmem_limit_bytes=VMEM)

    high, low = two_terms(sine_table(all_x)).astype(np.float32)
    table_x = np.concatenate([high, high, low], axis=1).reshape(rows, share_x, 3 * all_x)
    table_y = sine_table(all_y).reshape(cols, share_y, rows, part_y)
    table_y = np.einsum("cjry,ab->cajryb", table_y, np.eye(share_x, dtype=np.float32))
    table_y = table_y.reshape(cols, share_x * share_y, rows * share_x * part_y)
    table_z = sine_table(all_z).reshape(cols, part_z, all_z)
    table_y, table_z = two_terms(table_y), two_terms(table_z)

    pieces = pl.pallas_call(
        functools.partial(x_kernel, order=row_order),
        out_shape=[
            jax.ShapeDtypeStruct((len(ks) * share_x * part_y, width), jnp.float32)
            for ks in row_order
        ],
        in_specs=[hbm, hbm],
        out_specs=[vmem] * len(row_order),
        scratch_shapes=[
            pltpu.VMEM((fields, all_x * part_y, part_z), jnp.float32),
            pltpu.VMEM(table_x.shape, jnp.float32),
            pltpu.SemaphoreType.DMA((fields + 1,)),
        ],
        compiler_params=params,
        name="x_modes",
    )(
        pltpu.with_memory_space_constraint(
            species.reshape(fields, all_x * part_y, part_z), pltpu.HBM
        ),
        pltpu.with_memory_space_constraint(jnp.asarray(table_x), pltpu.HBM),
    )
    pieces = exchange_rows(pieces, row_order, rows)

    block = jax.ShapeDtypeStruct((share_x * share_y, width), jnp.float32)
    line = pltpu.VMEM((rows, share_x * part_y, width), jnp.bfloat16)
    blocks = pl.pallas_call(
        functools.partial(y_kernel, row_order=list(pieces), col_steps=col_steps),
        out_shape=[block] * cols,
        in_specs=[vmem] * (rows + 1),
        out_specs=[vmem] * cols,
        scratch_shapes=[line, line],
        compiler_params=params,
        name="y_modes",
    )(*pieces.values(), table_y)
    blocks = exchange_cols(blocks, col_steps, rows, cols)

    inverse = pl.pallas_call(
        symbol_kernel,
        out_shape=jax.ShapeDtypeStruct((share_x, share_y, all_z), jnp.float32),
        in_specs=[smem, smem, vmem],
        out_specs=vmem,
        compiler_params=params,
        name="inverse_symbol",
    )(symbol_x, symbol_y, symbol_z[None])
    return pl.pallas_call(
        functools.partial(z_kernel, col_steps=col_steps, fields=fields),
        out_shape=jax.ShapeDtypeStruct((fields, share_x, share_y, all_z), jnp.float32),
        in_specs=[vmem] * (cols + 2),
        out_specs=hbm,
        scratch_shapes=[
            pltpu.VMEM((fields, share_x, share_y, all_z), jnp.float32),
            pltpu.SemaphoreType.DMA((fields,)),
        ],
        compiler_params=params,
        name="z_modes",
    )(*blocks, inverse, table_z)


def plain_transform(values, dim):
    table = jnp.asarray(sine_table(values.shape[dim]))
    moved = jnp.tensordot(values, table, axes=([dim], [0]), precision=lax.Precision.HIGHEST)
    return jnp.moveaxis(moved, -1, dim)


def plain(species, symbol_x, symbol_y, symbol_z):
    values = plain_transform(species, 1)
    values = lax.all_to_all(values, "row", split_axis=1, concat_axis=2, tiled=True)
    values = plain_transform(values, 2)
    values = lax.all_to_all(values, "col", split_axis=2, concat_axis=3, tiled=True)
    values = plain_transform(values, 3)
    share_x, share_y = values.shape[1], values.shape[2]
    part_x = lax.dynamic_slice_in_dim(symbol_x, lax.axis_index("row") * share_x, share_x)
    part_y = lax.dynamic_slice_in_dim(symbol_y, lax.axis_index("col") * share_y, share_y)
    return values / (part_x[:, None, None] + part_y[None, :, None] + symbol_z)


def solution(mesh):
    rows, cols = mesh.shape["row"], mesh.shape["col"]

    def on_device(species, symbol_x, symbol_y, symbol_z):
        direct = all(n <= DIRECT and n & (n - 1) == 0 for n in (rows, cols))
        if direct and species.shape[3] * species.shape[0] % LANES == 0:
            return fast(species, symbol_x, symbol_y, symbol_z, rows=rows, cols=cols)
        return plain(species, symbol_x, symbol_y, symbol_z)

    return jax.shard_map(
        on_device,
        mesh=mesh,
        in_specs=(P(None, None, "row", "col"), P(), P(), P()),
        out_specs=P(None, "row", "col", None),
        check_vma=False,
    )
```

```python
import functools

import jax
import jax.numpy as jnp
import numpy as np
from jax import lax
from jax.experimental import pallas as pl
from jax.experimental.pallas import tpu as pltpu
from jax.sharding import PartitionSpec as P


LANES = 128
VMEM = 6 << 20
DIRECT = 16


def sine_table(count):
    rank = np.arange(1, count + 1)
    angle = np.pi / (count + 1) * (np.outer(rank, rank) % (2 * count + 2))
    return (np.sin(angle) * np.sqrt(2.0 / (count + 1))).astype(np.float32)


def two_terms(table):
    high = table.astype(jnp.bfloat16)
    low = (table - high.astype(np.float32)).astype(jnp.bfloat16)
    return np.stack([high, low])


def split(values):
    high = values.astype(jnp.bfloat16)
    low = (values - high.astype(jnp.float32)).astype(jnp.bfloat16)
    return high, low


def dot(left, right):
    return lax.dot_general(
        left, right, (((1,), (0,)), ((), ())), preferred_element_type=jnp.float32
    )


def dot3(left, right):
    return dot(left[0], right[0]) + dot(left[0], right[1]) + dot(left[1], right[0])


def round_trips(cols):
    gray = [i ^ (i >> 1) for i in range(cols)]
    cycles = gray, list(range(cols))
    return [
        tuple(tuple(c[(c.index(i) + n) % cols] for i in range(cols)) for c in cycles)
        for n in range(cols)
    ]


def look(table, at):
    found = jnp.int32(table[0])
    for i in range(1, len(table)):
        found = jnp.where(at == i, jnp.int32(table[i]), found)
    return found


def target(step, me_r, me_c):
    return jnp.where(me_r % 2 == 0, look(step[0], me_c), look(step[1], me_c))


def source(step, me_r, me_c):
    back = [tuple(table.index(i) for i in range(len(table))) for table in step]
    return target(back, me_r, me_c)


def x_kernel(species_ref, table_ref, *refs, order):
    out_refs, (a_ref, t_ref, sems) = refs[: len(order)], refs[len(order) :]
    me = lax.axis_index("row")
    fields = a_ref.shape[0]
    table = pltpu.make_async_copy(table_ref, t_ref, sems.at[fields])
    table.start()
    copies = [
        pltpu.make_async_copy(species_ref.at[f], a_ref.at[f], sems.at[f]) for f in range(fields)
    ]
    for copy in copies:
        copy.start()
    share, all_x = t_ref.shape[1], t_ref.shape[2] // 3
    part_y = a_ref.shape[1] // all_x
    table.wait()
    left = jnp.concatenate([t_ref[me ^ k] for ks in order for k in ks], axis=0)
    left = left.astype(jnp.bfloat16)
    for copy in copies:
        copy.wait()
    for y in range(part_y):
        rows = pl.ds(y, all_x, stride=part_y)
        high, low = split(jnp.concatenate([a_ref[f, rows, :] for f in range(fields)], axis=-1))
        out = dot(left, jnp.concatenate([high, low, high], axis=0))
        n = 0
        for ref, ks in zip(out_refs, order):
            for h in range(len(ks)):
                at = (h * part_y + y) * share
                ref[at : at + share] = out[n * share : (n + 1) * share]
                n += 1


def y_product(out_refs, right_refs, t_ref, steps):
    me_r, me_c = lax.axis_index("row"), lax.axis_index("col")
    to = [target(step, me_r, me_c) for step in steps]
    left = tuple(jnp.concatenate([t_ref[i, c] for c in to], axis=0) for i in range(2))
    right = tuple(r[...].reshape(-1, r.shape[-1]) for r in right_refs)
    out = dot3(left, right)
    share = out.shape[0] // len(out_refs)
    for n, ref in enumerate(out_refs):
        ref[...] = out[n * share : (n + 1) * share]


def y_kernel(*refs, row_order, steps):
    count = len(row_order)
    piece_refs, t_ref = refs[:count], refs[count]
    *out_refs, ch_ref, cl_ref = refs[count + 1 :]
    me = lax.axis_index("row")
    size = ch_ref.shape[1]
    for k, ref in zip(row_order, piece_refs):
        high, low = split(ref[ref.shape[0] - size :])
        ch_ref[me ^ k] = high
        cl_ref[me ^ k] = low
    y_product(out_refs, (ch_ref, cl_ref), t_ref, steps)


def own_kernel(ch_ref, cl_ref, t_ref, out_ref, *, step):
    y_product((out_ref,), (ch_ref, cl_ref), t_ref, [step])


def symbol_kernel(sx_ref, sy_ref, sz_ref, out_ref):
    share_x, share_y = out_ref.shape[0], out_ref.shape[1]
    at_x = lax.axis_index("row") * share_x
    at_y = lax.axis_index("col") * share_y
    place = lax.broadcasted_iota(jnp.int32, (share_y, 1), 0)
    part_y = jnp.zeros((share_y, 1), jnp.float32)
    for j in range(share_y):
        part_y = jnp.where(place == j, sy_ref[at_y + j], part_y)
    yz = part_y + sz_ref[...]
    for i in range(share_x):
        out_ref[i] = 1.0 / (yz + sx_ref[at_x + i])


def z_kernel(*refs, col_steps, fields):
    cols = len(col_steps)
    piece_refs = refs[:cols]
    inverse_ref, t_ref, out_ref, o_ref, sems = refs[cols:]
    me_r, me_c = lax.axis_index("row"), lax.axis_index("col")
    share_x, share_y, all_z = inverse_ref.shape
    part = piece_refs[0].shape[-1] // fields
    by = [source(step, me_r, me_c) for step in col_steps]
    right = tuple(jnp.concatenate([t_ref[i, c] for c in by], axis=0) for i in range(2))
    inverse = inverse_ref[...]
    copies = []
    step = 2 - fields % 2
    for f in range(0, fields, step):
        a = jnp.concatenate(
            [
                jnp.concatenate([r[:, g * part : (g + 1) * part] for r in piece_refs], axis=-1)
                for g in range(f, f + step)
            ],
            axis=0,
        )
        here = pl.ds(f, step)
        o_ref[here] = dot3(split(a), right).reshape(step, share_x, share_y, all_z) * inverse
        copies.append(pltpu.make_async_copy(o_ref.at[here], out_ref.at[here], sems.at[f]))
        copies[-1].start()
    for copy in copies:
        copy.wait()


def exchange_cols(blocks, steps, rows, cols):
    got = [blocks[0]]
    for step, block in zip(steps[1:], blocks[1:]):
        pairs = [(r * cols + c, r * cols + step[r % 2][c]) for r in range(rows) for c in range(cols)]
        got.append(lax.ppermute(block, ("row", "col"), pairs))
    return got


def exchange_rows(pieces, order, rows):
    here = {0: pieces[0]}
    size = pieces[0].shape[0]

    def send(piece, k):
        return lax.ppermute(piece, "row", [(i, i ^ k) for i in range(rows)])

    for ks, piece in zip(order[1:], pieces[1:]):
        here[ks[-1]] = send(piece, ks[-1])
    for ks in order[1:]:
        if len(ks) == 2:
            here[ks[0]] = send(here[ks[-1]][:size], 1)
    return here


def fast(species, symbol_x, symbol_y, symbol_z, *, rows, cols):
    fields, all_x, part_y, part_z = species.shape
    all_y, all_z = part_y * rows, part_z * cols
    share_x, share_y = all_x // rows, all_y // cols
    width = fields * part_z
    row_order = [(0,), *((k ^ 1, k) for k in range(5, rows, 2))]
    row_order += [(k,) for k in (3, 1, 2) if k < rows]
    col_steps = round_trips(cols)
    vmem = pl.BlockSpec(memory_space=pltpu.VMEM)
    smem = pl.BlockSpec(memory_space=pltpu.SMEM)
    hbm = pl.BlockSpec(memory_space=pltpu.HBM)
    params = pltpu.CompilerParams(vmem_limit_bytes=VMEM)

    high, low = two_terms(sine_table(all_x)).astype(np.float32)
    table_x = np.concatenate([high, high, low], axis=1).reshape(rows, share_x, 3 * all_x)
    table_y = sine_table(all_y).reshape(cols, share_y, rows, part_y)
    table_y = np.einsum("cjry,ab->cajryb", table_y, np.eye(share_x, dtype=np.float32))
    table_y = table_y.reshape(cols, share_x * share_y, rows * share_x * part_y)
    table_z = sine_table(all_z).reshape(cols, part_z, all_z)
    table_y, table_z = two_terms(table_y), two_terms(table_z)

    pieces = pl.pallas_call(
        functools.partial(x_kernel, order=row_order),
        out_shape=[
            jax.ShapeDtypeStruct((len(ks) * share_x * part_y, width), jnp.float32)
            for ks in row_order
        ],
        in_specs=[hbm, hbm],
        out_specs=[vmem] * len(row_order),
        scratch_shapes=[
            pltpu.VMEM((fields, all_x * part_y, part_z), jnp.float32),
            pltpu.VMEM(table_x.shape, jnp.float32),
            pltpu.SemaphoreType.DMA((fields + 1,)),
        ],
        compiler_params=params,
        name="x_modes",
    )(
        pltpu.with_memory_space_constraint(
            species.reshape(fields, all_x * part_y, part_z), pltpu.HBM
        ),
        pltpu.with_memory_space_constraint(jnp.asarray(table_x), pltpu.HBM),
    )
    pieces = exchange_rows(pieces, row_order, rows)

    block = jax.ShapeDtypeStruct((share_x * share_y, width), jnp.float32)
    line = jax.ShapeDtypeStruct((rows, share_x * part_y, width), jnp.bfloat16)
    *blocks, high, low = pl.pallas_call(
        functools.partial(y_kernel, row_order=list(pieces), steps=col_steps[1:]),
        out_shape=[block] * (cols - 1) + [line, line],
        in_specs=[vmem] * (rows + 1),
        out_specs=[vmem] * (cols + 1),
        compiler_params=params,
        name="y_modes",
    )(*pieces.values(), table_y)
    own = pl.pallas_call(
        functools.partial(own_kernel, step=col_steps[0]),
        out_shape=block,
        in_specs=[vmem] * 3,
        out_specs=vmem,
        compiler_params=params,
        name="y_own",
    )(high, low, table_y)
    blocks = [own, *blocks]
    blocks = exchange_cols(blocks, col_steps, rows, cols)

    inverse = pl.pallas_call(
        symbol_kernel,
        out_shape=jax.ShapeDtypeStruct((share_x, share_y, all_z), jnp.float32),
        in_specs=[smem, smem, vmem],
        out_specs=vmem,
        compiler_params=params,
        name="inverse_symbol",
    )(symbol_x, symbol_y, symbol_z[None])
    return pl.pallas_call(
        functools.partial(z_kernel, col_steps=col_steps, fields=fields),
        out_shape=jax.ShapeDtypeStruct((fields, share_x, share_y, all_z), jnp.float32),
        in_specs=[vmem] * (cols + 2),
        out_specs=hbm,
        scratch_shapes=[
            pltpu.VMEM((fields, share_x, share_y, all_z), jnp.float32),
            pltpu.SemaphoreType.DMA((fields,)),
        ],
        compiler_params=params,
        name="z_modes",
    )(*blocks, inverse, table_z)


def plain_transform(values, dim):
    table = jnp.asarray(sine_table(values.shape[dim]))
    moved = jnp.tensordot(values, table, axes=([dim], [0]), precision=lax.Precision.HIGHEST)
    return jnp.moveaxis(moved, -1, dim)


def plain(species, symbol_x, symbol_y, symbol_z):
    values = plain_transform(species, 1)
    values = lax.all_to_all(values, "row", split_axis=1, concat_axis=2, tiled=True)
    values = plain_transform(values, 2)
    values = lax.all_to_all(values, "col", split_axis=2, concat_axis=3, tiled=True)
    values = plain_transform(values, 3)
    share_x, share_y = values.shape[1], values.shape[2]
    part_x = lax.dynamic_slice_in_dim(symbol_x, lax.axis_index("row") * share_x, share_x)
    part_y = lax.dynamic_slice_in_dim(symbol_y, lax.axis_index("col") * share_y, share_y)
    return values / (part_x[:, None, None] + part_y[None, :, None] + symbol_z)


def solution(mesh):
    rows, cols = mesh.shape["row"], mesh.shape["col"]

    def on_device(species, symbol_x, symbol_y, symbol_z):
        direct = all(n <= DIRECT and n & (n - 1) == 0 for n in (rows, cols))
        if direct and species.shape[3] * species.shape[0] % LANES == 0:
            return fast(species, symbol_x, symbol_y, symbol_z, rows=rows, cols=cols)
        return plain(species, symbol_x, symbol_y, symbol_z)

    return jax.shard_map(
        on_device,
        mesh=mesh,
        in_specs=(P(None, None, "row", "col"), P(), P(), P()),
        out_specs=P(None, "row", "col", None),
        check_vma=False,
    )
```
